32 devices in a mesh: seq: 16 (over z, x, core), head: 1, batch: 2 (over y).
Axes of the slice: x: 2, y: 2, z: 4, core: 2. Of those that a mesh axis runs over, the one named last changes fastest.
Arguments:
- queries: bfloat16 [2, 8192, 8, 8, 128], P('batch', 'seq', 'head'), may hold values from -160 to 160
- key_rows: bfloat16 [2, 8192, 8, 128], P('batch', 'seq'), may hold values from -6 to 6
- value_rows: bfloat16 [2, 8192, 8, 128], P('batch', 'seq'), may hold values from -6 to 6
- compressed: bfloat16 [2, 128, 8, 128], P('batch', 'seq'), may hold values from -6 to 6
- chosen: int32 [2, 128, 8, 16], P('batch', 'seq'), may hold values from 0 to 127, as said below
Outputs:
- block_scores: float32 [2, 128, 8, 128], P('batch', 'seq', 'head')
- attended: bfloat16 [2, 8192, 8, 8, 128], P('batch', 'seq', 'head')
The draws below stay inside these ranges and needn't reach their ends.
Inputs may be any that keep to these rules, and one draw needn't show every extreme that they name: `chosen`: every entry is at most its own tile number, and entry 0 of every row is the tile's own block. Over the tiles of one device of seq and one group, at most 2 different blocks of any other device are named, and every device after the first names exactly 2 blocks of the first device for each group.
All inputs are finite; a program needn't handle non-finite values.
Results may differ from the reference program's by a relative error of at most 0.008.
Values may be sent and summed in bfloat16 or wider, within the bound.
A program may use at most 128 MiB of HBM per device.

```python
import jax
import jax.numpy as jnp
from jax import lax

HPG = 8
G = 8
DH = 128
BLOCK = 64
TOPN = 16
BATCH = 2
SEQ_LEN = 8192
BLK_DEV = 8
NBLK = 128


def fields(key):
    key_one, key_two, key_three = jax.random.split(jax.random.fold_in(key, 71), 3)
    key_base = jnp.clip(jax.random.normal(key_one, (BATCH, SEQ_LEN, G, DH), jnp.float32), -5.0, 5.0)
    comp_base = jnp.clip(jax.random.normal(key_two, (BATCH, NBLK, G, DH), jnp.float32), -5.0, 5.0)
    query_base = jnp.clip(jax.random.normal(key_three, (BATCH, SEQ_LEN, HPG, G, DH), jnp.float32), -5.0, 5.0)
    return (query_base, key_base, comp_base)


def draw_queries(key, part):
    return fields(key)[0].astype(jnp.bfloat16)


def draw_key_rows(key, part):
    return fields(key)[1].astype(jnp.bfloat16)


def draw_compressed(key, part):
    return fields(key)[2].astype(jnp.bfloat16)


def draw_chosen(key, part):
    key_one, key_two, key_three = jax.random.split(jax.random.fold_in(key, 5), 3)
    shards = NBLK // BLK_DEV
    lower_pick = jax.random.randint(key_one, (BATCH, shards, G, shards), 0, BLK_DEV)
    upper_pick = (lower_pick + 1 + jax.random.randint(key_two, (BATCH, shards, G, shards), 0, BLK_DEV - 1)) % BLK_DEV
    offsets = jnp.arange(shards, dtype=jnp.int32) * BLK_DEV
    candidates = jnp.stack([lower_pick + offsets, upper_pick + offsets], axis=-1).reshape(BATCH, shards, G, shards * 2)
    tile_ids = jnp.arange(NBLK, dtype=jnp.int32)
    span_ids = tile_ids // BLK_DEV
    inner_ids = tile_ids % BLK_DEV
    remote_count = 2 * span_ids
    pool_size = remote_count + inner_ids + 1
    random_pointer = jax.random.randint(key_three, (BATCH, NBLK, G, TOPN), 0, pool_size[None, :, None, None])
    slot_ids = jnp.arange(TOPN, dtype=jnp.int32)[None, None, None, :]
    own_pointer = (remote_count + inner_ids)[None, :, None, None]
    sink_pointer = (inner_ids % 2)[None, :, None, None]
    has_remote = (span_ids > 0)[None, :, None, None]
    pointer = jnp.where(slot_ids == 0, own_pointer, jnp.where((slot_ids == 1) & has_remote, sink_pointer, random_pointer))
    tile_candidates = candidates[:, span_ids]
    remote_ids = jnp.take_along_axis(tile_candidates, jnp.clip(pointer, 0, shards * 2 - 1), axis=-1)
    local_ids = (span_ids * BLK_DEV - remote_count)[None, :, None, None] + pointer
    return jnp.where(pointer < remote_count[None, :, None, None], remote_ids, local_ids).astype(jnp.int32)


def levels(key, extent, pieces, least, top_value):
    gain = 1.0
    for position, parts in pieces:
        draws = jax.random.uniform(jax.random.fold_in(jax.random.fold_in(key, 6), position), (parts,), jnp.float32, least / len(pieces), top_value / len(pieces))
        gain = gain * jnp.repeat(jnp.exp(draws), extent[position] // parts).reshape((-1,) + (1,) * (len(extent) - 1 - position))
    return gain


def gaussian(key, shape, scale, most, pieces=(), kind=jnp.bfloat16):
    result = scale * jax.random.normal(key, shape, jnp.float32)
    if pieces:
        result = result * levels(key, shape, pieces, -0.22, 0.18)
    return jnp.clip(result, -most, most).astype(kind)


def setup_inputs(seed: int = 0) -> dict:
    key_of = jax.random.split(jax.random.key(seed), 6)
    return {
        "queries": draw_queries(jax.random.fold_in(key_of[5], 71), 0),
        "key_rows": draw_key_rows(jax.random.fold_in(key_of[5], 71), 0),
        "value_rows": gaussian(key_of[2], (BATCH, SEQ_LEN, G, DH), 1.0, 6.0, ((0, 2), (1, 16))),
        "compressed": draw_compressed(jax.random.fold_in(key_of[5], 71), 0),
        "chosen": draw_chosen(jax.random.fold_in(key_of[5], 71), 0),
    }


def softmax_parts(scores):
    row_top = jnp.max(scores, axis=-1, keepdims=True)
    weights = jnp.exp(scores - row_top)
    return weights, jnp.sum(weights, axis=-1, keepdims=True)


def one_sequence(inputs):
    query_seq, key_seq, value_seq, compressed_seq, chosen_seq = inputs
    score_scale = DH ** -0.5
    tile_step = 2
    rounds = NBLK // tile_step
    key_blocks = key_seq.reshape(NBLK, BLOCK, G, DH)
    value_blocks = value_seq.reshape(NBLK, BLOCK, G, DH)
    all_blocks = jnp.arange(NBLK, dtype=jnp.int32)
    group_ids = jnp.arange(G, dtype=jnp.int32)[None, :, None]
    comp_wide = compressed_seq.astype(jnp.float32)

    def per_round(round_in):
        query_part, pick_part, round_id = round_in
        query_pos = round_id * (tile_step * BLOCK) + jnp.arange(tile_step * BLOCK, dtype=jnp.int32)
        query_wide = query_part.astype(jnp.float32)
        logits = jnp.einsum("qhgd,ngd->qhgn", query_wide, comp_wide) * score_scale
        seen = all_blocks[None, :] <= (query_pos // BLOCK)[:, None]
        logits = jnp.where(seen[:, None, None, :], logits, -jnp.inf)
        weights, totals = softmax_parts(logits)
        probability = weights / totals
        pooled = jnp.sum(probability.reshape(tile_step, BLOCK, HPG, G, NBLK), axis=(1, 2))
        tile_ids = round_id * tile_step + jnp.arange(tile_step, dtype=jnp.int32)
        factor = (tile_ids + 1).astype(jnp.float32) / (BLOCK * HPG)
        scores_out = pooled * factor[:, None, None]
        key_sel = key_blocks[pick_part, :, group_ids, :].reshape(tile_step, G, TOPN * BLOCK, DH)
        value_sel = value_blocks[pick_part, :, group_ids, :].reshape(tile_step, G, TOPN * BLOCK, DH)
        key_pos = (pick_part[..., None] * BLOCK + jnp.arange(BLOCK, dtype=jnp.int32)).reshape(tile_step, G, TOPN * BLOCK)
        query_tiles = query_wide.reshape(tile_step, BLOCK, HPG, G, DH)
        scores = jnp.einsum("tqhgd,tgkd->tghqk", query_tiles, key_sel.astype(jnp.float32)) * score_scale
        tile_pos = query_pos.reshape(tile_step, BLOCK)
        visible = key_pos[:, :, None, None, :] <= tile_pos[:, None, None, :, None]
        scores = jnp.where(visible, scores, -jnp.inf)
        weights, totals = softmax_parts(scores)
        rounded = weights.astype(jnp.bfloat16)
        mixed = jnp.einsum("tghqk,tgkd->tqhgd", rounded.astype(jnp.float32), value_sel.astype(jnp.float32))
        attended = (mixed / jnp.transpose(totals, (0, 3, 2, 1, 4))).astype(jnp.bfloat16)
        return scores_out, attended.reshape(tile_step * BLOCK, HPG, G, DH)

    round_ids = jnp.arange(rounds, dtype=jnp.int32)
    scores_out, attended = lax.map(per_round, (query_seq.reshape(rounds, tile_step * BLOCK, HPG, G, DH), chosen_seq.reshape(rounds, tile_step, G, TOPN), round_ids))
    return scores_out.reshape(NBLK, G, NBLK), attended.reshape(SEQ_LEN, HPG, G, DH)


def reference(queries, key_rows, value_rows, compressed, chosen):
    block_scores, attended = lax.map(one_sequence, (queries, key_rows, value_rows, compressed, chosen))
    return block_scores, attended
```

```python
import functools
import math

import jax
import jax.numpy as jnp
from jax import lax
from jax.experimental import pallas as pl
from jax.experimental.pallas import tpu as pltpu
from jax.sharding import PartitionSpec as P

HPG = 8
BLOCK = 64
TOPN = 16
CAP = 2


def softmax_parts(scores):
    row_top = jnp.max(scores, axis=-1, keepdims=True)
    weights = jnp.exp(scores - row_top)
    return (weights, jnp.sum(weights, axis=-1, keepdims=True))


def attend_tile(shape, slot_ref, pick_ref, first_ref, query_ref, own_ref, remote_ref, out_ref, pool, picked):
    heads_local, blk_dev, shards, cap, block_len, head_width = shape
    group, tile = pl.program_id(0), pl.program_id(1)

    @pl.when(tile == 0)
    def _():
        pool[:blk_dev] = own_ref[0]
        for shard in range(shards):
            pool[blk_dev + shard * cap : blk_dev + (shard + 1) * cap] = remote_ref[shard, 0]

    tile_number = first_ref[0] + tile
    keys = TOPN * block_len
    column = lax.broadcasted_iota(jnp.int32, (1, keys), 1)
    within = column % block_len
    block_place = column // block_len
    limit = jnp.full((1, keys), -1, jnp.int32)
    for place in range(TOPN):
        picked[place * block_len : (place + 1) * block_len] = pool[slot_ref[tile, group, place]]
        is_own = pick_ref[tile, group, place] == tile_number
        limit = jnp.where((block_place == place) & is_own, within, limit)
    rows = block_len * heads_local
    part = min(rows, 256)
    factor = math.log2(math.e) * head_width ** (-0.5)
    for start in range(0, rows, part):
        query = query_ref[0, 0, start : start + part]
        scores = lax.dot_general(
            query,
            picked[:, :head_width],
            (((1,), (1,)), ((), ())),
            preferred_element_type=jnp.float32,
        )
        token = (start + lax.broadcasted_iota(jnp.int32, (part, 1), 0)) // heads_local
        scores = jnp.where(limit <= token, scores, -jnp.inf)
        row_top = jnp.max(scores, axis=-1, keepdims=True)
        weights = jnp.exp2((scores - row_top) * factor)
        totals = jnp.sum(weights, axis=-1, keepdims=True)
        mixed = jnp.dot(
            weights.astype(jnp.bfloat16),
            picked[:, head_width:],
            preferred_element_type=jnp.float32,
        )
        out_ref[0, 0, start : start + part] = (mixed / totals).astype(jnp.bfloat16)


def local(queries, key_rows, value_rows, compressed, chosen):
    _, tok_rows, heads_local, groups, head_width = queries.shape
    block_len = BLOCK
    shards = lax.axis_size("seq")
    seq_rank = lax.axis_index("seq")
    blk_dev = tok_rows // block_len
    nblk = blk_dev * shards
    score_scale = head_width ** (-0.5)
    query_rows = queries[0]
    query_pos = seq_rank * tok_rows + jnp.arange(tok_rows, dtype=jnp.int32)
    gathered = lax.all_gather(compressed, "seq", axis=1, tiled=True)
    logits = (
        jnp.einsum(
            "tjgd,ngd->tjgn",
            query_rows,
            gathered[0],
            preferred_element_type=jnp.float32,
        )
        * score_scale
    )
    all_blocks = jnp.arange(nblk, dtype=jnp.int32)
    seen = all_blocks[None, :] <= (query_pos // block_len)[:, None]
    logits = jnp.where(seen[:, None, None, :], logits, -jnp.inf)
    weights, totals = softmax_parts(logits)
    probability = weights / totals
    pooled = jnp.sum(
        probability.reshape(blk_dev, block_len, heads_local, groups, nblk), axis=(1, 2)
    )[None]
    shared = lax.psum_scatter(
        pooled.astype(jnp.bfloat16), "head", scatter_dimension=2, tiled=True
    ).astype(jnp.float32)
    tile_ids = seq_rank * blk_dev + jnp.arange(blk_dev, dtype=jnp.int32)
    factor = (tile_ids + 1).astype(jnp.float32) / (block_len * HPG)
    block_scores = shared * factor[None, :, None, None]
    pick_rows = chosen[0]
    onehot = pick_rows[..., None] == all_blocks
    needed = jnp.any(onehot, axis=(0, 2))
    owner_of = all_blocks // blk_dev
    needed = needed & (owner_of != seq_rank)[None, :]
    needed_grid = needed.reshape(groups, shards, blk_dev).astype(jnp.int32)
    rank_in = jnp.cumsum(needed_grid, axis=2) - needed_grid
    places = jnp.arange(CAP, dtype=jnp.int32)
    within = jnp.arange(blk_dev, dtype=jnp.int32)
    matched = (needed_grid[..., None] == 1) & (rank_in[..., None] == places)
    wanted = jnp.sum(jnp.where(matched, within[:, None], 0), axis=2)
    slot_of = blk_dev + owner_of[None, :] * CAP + rank_in.reshape(groups, nblk)
    slot_of = jnp.where(
        owner_of[None, :] == seq_rank, all_blocks[None, :] - seq_rank * blk_dev, slot_of
    )
    pool_index = jnp.sum(jnp.where(onehot, slot_of[None, :, None, :], 0), axis=3)
    key_local = key_rows[0].reshape(blk_dev, block_len, groups, head_width)
    value_local = value_rows[0].reshape(blk_dev, block_len, groups, head_width)
    own_rows = jnp.transpose(jnp.concatenate([key_local, value_local], axis=-1), (2, 0, 1, 3))
    requested = lax.all_to_all(
        jnp.transpose(wanted, (1, 0, 2)), "seq", split_axis=0, concat_axis=0, tiled=True
    )
    group_ids = jnp.arange(groups, dtype=jnp.int32)[None, :, None]
    found = jnp.take(
        own_rows.reshape(groups * blk_dev, block_len, 2 * head_width),
        group_ids * blk_dev + requested,
        axis=0,
        mode="clip",
    )
    found, _ = lax.optimization_barrier((found, gathered))
    fetched = lax.all_to_all(found, "seq", split_axis=0, concat_axis=0, tiled=True)
    rows = block_len * heads_local
    query_tiles = jnp.transpose(
        query_rows.reshape(blk_dev, rows, groups, head_width), (2, 0, 1, 3)
    )
    shape = (heads_local, blk_dev, shards, CAP, block_len, head_width)
    tile_spec = pl.BlockSpec((1, 1, rows, head_width), lambda g, t, *_: (g, t, 0, 0))
    attended = pl.pallas_call(
        functools.partial(attend_tile, shape),
        grid_spec=pltpu.PrefetchScalarGridSpec(
            num_scalar_prefetch=3,
            grid=(groups, blk_dev),
            in_specs=[
                tile_spec,
                pl.BlockSpec(
                    (1, blk_dev, block_len, 2 * head_width), lambda g, t, *_: (g, 0, 0, 0)
                ),
                pl.BlockSpec(
                    (shards, 1, CAP, block_len, 2 * head_width),
                    lambda g, t, *_: (0, g, 0, 0, 0),
                ),
            ],
            out_specs=tile_spec,
            scratch_shapes=[
                pltpu.VMEM((blk_dev + shards * CAP, block_len, 2 * head_width), jnp.bfloat16),
                pltpu.VMEM((TOPN * block_len, 2 * head_width), jnp.bfloat16),
            ],
        ),
        out_shape=jax.ShapeDtypeStruct((groups, blk_dev, rows, head_width), jnp.bfloat16),
        compiler_params=pltpu.CompilerParams(
            dimension_semantics=("arbitrary", "arbitrary"), vmem_limit_bytes=48 * 1024 * 1024
        ),
    )(pool_index, pick_rows, (seq_rank * blk_dev)[None], query_tiles, own_rows, fetched)
    attended = jnp.transpose(attended, (1, 2, 0, 3))
    attended = attended.reshape(1, tok_rows, heads_local, groups, head_width)
    return (block_scores, attended)


def solution(mesh):
    placed = (
        P("batch", "seq", "head", None, None),
        P("batch", "seq", None, None),
        P("batch", "seq", None, None),
        P("batch", "seq", None, None),
        P("batch", "seq", None, None),
    )
    return jax.shard_map(
        local,
        mesh=mesh,
        in_specs=placed,
        out_specs=(P("batch", "seq", "head", None), P("batch", "seq", "head", None, None)),
        check_vma=False,
    )
```
